32 devices in a mesh: seq: 16 (over z, y, x), head: 2 (over core).
Axes of the slice: x: 2, y: 2, z: 4, core: 2. Of those that a mesh axis runs over, the one named last changes fastest.
Arguments:
- queries: bfloat16 [4096, 3584], P('seq', 'head'), may hold values from -5 to 5
- keys: bfloat16 [4096, 3584], P('seq', 'head'), may hold values from -5 to 5
- values: bfloat16 [4096, 3584], P('seq', 'head'), may hold values from -6 to 6
- attn_grad: bfloat16 [4096, 3584], P('seq', 'head'), may hold values from -6 to 6
- doc_ids: int32 [4096], replicated, may hold values from 0 to 3, never falling along the last dimension, each value on 1 to 2048 neighbouring positions
- conv_input: bfloat16 [4096, 7168], P('seq', 'head'), may hold values from -6 to 6
- conv_weight: float32 [4, 7168], P(None, 'head'), may hold values from -3 to 3
- step_raw: float32 [4096, 112], P('seq', 'head'), may hold values from -4 to 4
- step_bias: float32 [112], P('head'), may hold values from -1.5 to 0
- rate_log: float32 [112], P('head'), may hold values from -13 to -1
- skip_gain: float32 [112], P('head'), may hold values from 0.5 to 1.5
- input_coeff: bfloat16 [4096, 128], P('seq'), may hold values from -0.625 to 0.625
- output_coeff: bfloat16 [4096, 128], P('seq'), may hold values from -0.625 to 0.625
- gate_input: bfloat16 [4096, 7168], P('seq', 'head'), may hold values from -6 to 6
- mix_grad: bfloat16 [4096, 7168], P('seq', 'head'), may hold values from -1.5 to 1.5
Outputs:
- grad_queries: bfloat16 [4096, 3584], P('seq', 'head')
- grad_keys: bfloat16 [4096, 3584], P('seq', 'head')
- grad_values: bfloat16 [4096, 3584], P('seq', 'head')
- grad_conv_input: bfloat16 [4096, 7168], P('seq', 'head')
- grad_gate: bfloat16 [4096, 7168], P('seq', 'head')
- grad_step: float32 [4096, 112], P('seq', 'head')
- grad_input_coeff: float32 [4096, 128], P('seq')
- grad_output_coeff: float32 [4096, 128], P('seq')
- grad_conv_weight: float32 [4, 7168], P(None, 'head')
- grad_step_bias: float32 [112], P('head')
- grad_rate_log: float32 [112], P('head')
- grad_skip: float32 [112], P('head')
The draws below stay inside these ranges and needn't reach their ends.
Inputs may be any that keep to these rules, and one draw needn't show every extreme that they name: doc_ids never fall along the sequence.
All inputs are finite; a program needn't handle non-finite values.
Results may differ from the reference program's by a relative error of at most 0.012.
Values may be sent and summed in bfloat16 or wider, within the bound.
A program may use at most 192 MiB of HBM per device.

```python
import math
import jax
import jax.numpy as jnp
import numpy as np
from jax import lax

T_DEV = 256
HEADS = 16
HEAD_DIM = 224
WINDOW = 1024
SSM_HEADS = 112
SSM_DIM = 64
STATE = 64
GROUPS = 2
KERNEL = 4
STRETCH = 128
SEQLEN = 4096
INNER = 7168
DOCS = 4


def aligned_pair(key):
    shape = (SEQLEN, HEADS * HEAD_DIM)
    normal_query = jax.random.truncated_normal(jax.random.fold_in(key, 11), -4.5, 4.5, shape, jnp.float32)
    normal_key = jax.random.truncated_normal(jax.random.fold_in(key, 12), -4.5, 4.5, shape, jnp.float32)
    return (normal_query, normal_key)


def draw_queries(key, part):
    return aligned_pair(key)[0].astype(jnp.bfloat16)


def draw_keys(key, part):
    return aligned_pair(key)[1].astype(jnp.bfloat16)


def draw_step_raw(key, part):
    blocks = SEQLEN // STRETCH
    offsets = jax.random.uniform(jax.random.fold_in(key, 21), (blocks, 1, SSM_HEADS), jnp.float32, -1.0, 1.0)
    noise = 0.5 * jax.random.truncated_normal(jax.random.fold_in(key, 23), -5.0, 5.0, (blocks, STRETCH, SSM_HEADS), jnp.float32)
    return (noise + offsets).reshape(SEQLEN, SSM_HEADS)


def draw_rate_log(key, part):
    chance = 0.5
    picked = jax.random.uniform(jax.random.fold_in(key, 31), (SSM_HEADS,), jnp.float32) < chance
    quick = jnp.log(jax.random.uniform(jax.random.fold_in(key, 32), (SSM_HEADS,), jnp.float32, 0.05, 0.3))
    slowly = jnp.log(jax.random.uniform(jax.random.fold_in(key, 33), (SSM_HEADS,), jnp.float32, 0.3, 2.0) / SEQLEN)
    return jnp.where(picked, quick, slowly)


def level_of(rng, shape, cuts, least, top_value):
    factor_of = 1.0
    for dim, shards_of in cuts:
        steps = jax.random.uniform(jax.random.fold_in(jax.random.fold_in(rng, 6), dim), (shards_of,), jnp.float32, least / len(cuts), top_value / len(cuts))
        factor_of = factor_of * jnp.repeat(jnp.exp(steps), shape[dim] // shards_of).reshape((-1,) + (1,) * (len(shape) - 1 - dim))
    return factor_of


def length_profile(count, total, bound, skew):
    loads = [(1 << 20) // math.isqrt(standing ** skew) + 1 for standing in range(2, count + 1)]
    rest, holding = total - bound - (count - 1), [1] * (count - 1)
    while rest > 0:
        free = [i for i in range(count - 1) if holding[i] < bound]
        whole, left = sum([loads[i] for i in free]), rest
        for i in free:
            addition = min(bound - holding[i], max(1, left * loads[i] // whole), rest)
            holding[i] = holding[i] + addition
            rest = rest - addition
    return np.array([bound] + holding)


def ragged_sizes(rng, number_of, total, reach, slope):
    if number_of == 2:
        one = jax.random.randint(rng, (), max(1, total - reach), min(reach, total - 1) + 1)
        return jnp.stack([one, total - one])
    sizes = jnp.asarray(length_profile(number_of, total, reach, slope), jnp.int32)
    twos = (number_of - 1) // 2
    giver, sink = sizes[1:1 + 2 * twos:2], sizes[2:2 + 2 * twos:2]
    margin = jnp.minimum(giver - 1, reach - sink)
    moved = jax.random.randint(jax.random.fold_in(rng, 1), (twos,), 0, 1 << 20) % (margin + 1)
    sizes = sizes.at[1:1 + 2 * twos:2].set(giver - moved).at[2:2 + 2 * twos:2].set(sink + moved)
    return sizes[jax.random.permutation(jax.random.fold_in(rng, 2), number_of)]


def bell_draw(key, shape, scale, most, split=(), kind=jnp.bfloat16):
    entries = jax.random.normal(key, shape, jnp.float32) * scale
    if len(split) > 0:
        entries = level_of(key, shape, split, -0.22, 0.18) * entries
    return jnp.clip(entries, min=-most, max=most).astype(kind)


def setup_inputs(seed: int = 0) -> dict:
    arg_keys = jax.random.split(jax.random.key(seed), 16)
    queries = draw_queries(jax.random.fold_in(arg_keys[15], 71), 0)
    keys = draw_keys(jax.random.fold_in(arg_keys[15], 71), 0)
    values = bell_draw(arg_keys[2], (SEQLEN, HEADS * HEAD_DIM), 1.0, 6.0, ((0, 16), (1, 2)))
    attn_grad = bell_draw(arg_keys[3], (SEQLEN, HEADS * HEAD_DIM), 1.0, 6.0, ((0, 16), (1, 2)))
    doc_ids = jnp.searchsorted(jnp.cumsum(ragged_sizes(arg_keys[4], DOCS, SEQLEN, SEQLEN // 2, 2)), jnp.arange(SEQLEN), side="right").astype(jnp.int32)
    conv_input = bell_draw(arg_keys[5], (SEQLEN, INNER), 1.0, 6.0, ((0, 16), (1, 2)))
    conv_weight = bell_draw(arg_keys[6], (KERNEL, INNER), KERNEL ** -0.5, 3.0, ((1, 2),), jnp.float32)
    step_raw = draw_step_raw(jax.random.fold_in(arg_keys[15], 71), 0)
    step_bias = jnp.clip(-1.5 + 1.5 * jax.random.uniform(arg_keys[8], (SSM_HEADS,), jnp.float32) ** level_of(arg_keys[8], (SSM_HEADS,), ((0, 2),), -0.2, 0.2), -1.5, 0.0)
    rate_log = draw_rate_log(jax.random.fold_in(arg_keys[15], 71), 0)
    skip_gain = jnp.clip(0.5 + 1.0 * jax.random.uniform(arg_keys[10], (SSM_HEADS,), jnp.float32) ** level_of(arg_keys[10], (SSM_HEADS,), ((0, 2),), -0.2, 0.2), 0.5, 1.5)
    input_coeff = bell_draw(arg_keys[11], (SEQLEN, GROUPS * STATE), 0.1, 0.625, ((0, 16),))
    output_coeff = bell_draw(arg_keys[12], (SEQLEN, GROUPS * STATE), 0.1, 0.625, ((0, 16),))
    gate_input = bell_draw(arg_keys[13], (SEQLEN, INNER), 1.0, 6.0, ((0, 16), (1, 2)))
    mix_grad = bell_draw(arg_keys[14], (SEQLEN, INNER), 0.25, 1.5, ((0, 16), (1, 2)))
    return dict(queries=queries, keys=keys, values=values, attn_grad=attn_grad, doc_ids=doc_ids, conv_input=conv_input, conv_weight=conv_weight, step_raw=step_raw, step_bias=step_bias, rate_log=rate_log, skip_gain=skip_gain, input_coeff=input_coeff, output_coeff=output_coeff, gate_input=gate_input, mix_grad=mix_grad)


NEG_FILL = -1e+30
EXACT = lax.Precision.HIGHEST

def conv_act(padded, doc_ext, weight):
    kernel_taps = weight.shape[0]
    length = padded.shape[0] - kernel_taps + 1
    doc_now = doc_ext[kernel_taps - 1:]
    summed = jnp.zeros((length, padded.shape[1]), jnp.float32)
    for lagged in range(kernel_taps):
        first_row = kernel_taps - 1 - lagged
        shifted = padded[first_row:first_row + length]
        same_doc = doc_ext[first_row:first_row + length] == doc_now
        summed = summed + weight[lagged] * jnp.where(same_doc[:, None], shifted, 0.0)
    return jax.nn.silu(summed)

def stretch_layout(log_decay, doc_row, doc_before):
    blocks = doc_row.shape[0] // STRETCH
    cumulative = jnp.cumsum(log_decay.reshape(blocks, STRETCH), axis=1)
    doc_grid = doc_row.reshape(blocks, STRETCH)
    previous = jnp.concatenate([jnp.reshape(doc_before, (1,)), doc_grid[:-1, -1]])
    return (cumulative, doc_grid, previous)

def head_final(head_act, step_size, log_decay, in_grid, start_state, doc_row, doc_before):
    cumulative, doc_grid, previous = stretch_layout(log_decay, doc_row, doc_before)
    blocks = cumulative.shape[0]
    scaled = (head_act * step_size[:, None]).reshape(blocks, STRETCH, head_act.shape[1])
    same_end = doc_grid == doc_grid[:, -1:]
    to_end = jnp.where(same_end, jnp.exp(jnp.where(same_end, cumulative[:, -1:] - cumulative, 0.0)), 0.0)
    local_state = jnp.einsum('cjp,cjn->cpn', scaled * to_end[:, :, None], in_grid, precision=EXACT)
    through = jnp.where(doc_grid[:, -1] == previous, jnp.exp(cumulative[:, -1]), 0.0)

    def advance(carry_state, pair_item):
        return (pair_item[0] * carry_state + pair_item[1], carry_state)
    final_state, starts = lax.scan(advance, start_state, (through, local_state))
    return (final_state, starts, cumulative, doc_grid, previous, scaled)

def head_output(head_act, step_size, log_decay, pair_grid, in_grid, out_grid, gate_part, skip_gain, start_state, doc_row, doc_before):
    final_state, starts, cumulative, doc_grid, previous, scaled = head_final(head_act, step_size, log_decay, in_grid, start_state, doc_row, doc_before)
    causal = jnp.arange(STRETCH)[:, None] >= jnp.arange(STRETCH)[None, :]
    same_doc = (doc_grid[:, :, None] == doc_grid[:, None, :]) & causal[None]
    weights = jnp.where(same_doc, jnp.exp(jnp.where(same_doc, cumulative[:, :, None] - cumulative[:, None, :], 0.0)), 0.0)
    inner_part = jnp.einsum('cij,cjp->cip', pair_grid * weights, scaled, precision=EXACT)
    enter_gain = jnp.where(doc_grid == previous[:, None], jnp.exp(cumulative), 0.0)
    carried = jnp.einsum('cin,cpn->cip', out_grid, starts, precision=EXACT) * enter_gain[:, :, None]
    mixed_out = (inner_part + carried).reshape(head_act.shape) + skip_gain * head_act
    return (mixed_out * jax.nn.silu(gate_part), final_state)

def round_edge(term):
    edge = lax.optimization_barrier(term[:WINDOW].astype(jnp.bfloat16)).astype(jnp.float32)
    return jnp.concatenate([edge, term[WINDOW:]], axis=0)

def attention_grads(queries, keys, values, attn_grad, doc_ids):
    width = HEADS * HEAD_DIM
    span = WINDOW + T_DEV
    scale = HEAD_DIM ** (-0.5)
    key_pad = jnp.concatenate([jnp.zeros((WINDOW, width), keys.dtype), keys])
    value_pad = jnp.concatenate([jnp.zeros((WINDOW, width), values.dtype), values])
    doc_pad = jnp.concatenate([jnp.full((WINDOW,), -1, jnp.int32), doc_ids])
    distance = jnp.arange(T_DEV)[:, None] + WINDOW - jnp.arange(span)[None, :]
    in_window = (distance >= 0) & (distance < WINDOW)

    def one_block(carry, index):
        key_acc, value_acc = carry
        first_row = index * T_DEV
        query_part = lax.dynamic_slice_in_dim(queries, first_row, T_DEV).astype(jnp.float32).reshape(T_DEV, HEADS, HEAD_DIM)
        grad_part = lax.dynamic_slice_in_dim(attn_grad, first_row, T_DEV).astype(jnp.float32).reshape(T_DEV, HEADS, HEAD_DIM)
        key_part = lax.dynamic_slice_in_dim(key_pad, first_row, span).astype(jnp.float32).reshape(span, HEADS, HEAD_DIM)
        value_part = lax.dynamic_slice_in_dim(value_pad, first_row, span).astype(jnp.float32).reshape(span, HEADS, HEAD_DIM)
        doc_query = lax.dynamic_slice_in_dim(doc_ids, first_row, T_DEV)
        doc_key = lax.dynamic_slice_in_dim(doc_pad, first_row, span)
        allowed = in_window & (doc_query[:, None] == doc_key[None, :])
        scores = jnp.where(allowed[None], jnp.einsum('ihd,jhd->hij', query_part, key_part) * scale, NEG_FILL)
        row_max = lax.optimization_barrier(jnp.max(scores, axis=-1))
        expo = jnp.where(allowed[None], jnp.exp(scores - row_max[:, :, None]), 0.0)
        row_sum = lax.optimization_barrier(jnp.sum(expo, axis=-1))
        probs = expo / jnp.maximum(row_sum, 1.0)[:, :, None]
        probs_half = lax.optimization_barrier(probs.astype(jnp.bfloat16)).astype(jnp.float32)
        attn_out = jnp.einsum('hij,jhd->ihd', probs_half, value_part)
        delta = lax.optimization_barrier(jnp.sum(grad_part * attn_out, axis=-1)).T
        dprob = jnp.einsum('ihd,jhd->hij', grad_part, value_part)
        dscore = lax.optimization_barrier((probs * (dprob - delta[:, :, None])).astype(jnp.bfloat16)).astype(jnp.float32)
        grad_query = (jnp.einsum('hij,jhd->ihd', dscore, key_part) * scale).reshape(T_DEV, width).astype(jnp.bfloat16)
        key_term = round_edge(jnp.einsum('hij,ihd->jhd', dscore, query_part).reshape(span, width))
        value_term = round_edge(jnp.einsum('hij,ihd->jhd', probs_half, grad_part).reshape(span, width))
        key_acc = lax.dynamic_update_slice_in_dim(key_acc, lax.dynamic_slice_in_dim(key_acc, first_row, span) + key_term, first_row, 0)
        value_acc = lax.dynamic_update_slice_in_dim(value_acc, lax.dynamic_slice_in_dim(value_acc, first_row, span) + value_term, first_row, 0)
        return ((key_acc, value_acc), grad_query)
    zero_acc = jnp.zeros((WINDOW + SEQLEN, width), jnp.float32)
    (key_acc, value_acc), grad_blocks = lax.scan(one_block, (zero_acc, zero_acc), jnp.arange(SEQLEN // T_DEV, dtype=jnp.int32))
    grad_queries = grad_blocks.reshape(SEQLEN, width)
    grad_keys = (key_acc[WINDOW:] * scale).astype(jnp.bfloat16)
    grad_values = value_acc[WINDOW:].astype(jnp.bfloat16)
    return (grad_queries, grad_keys, grad_values)

def mixer_grads(doc_ids, conv_input, conv_weight, step_raw, step_bias, rate_log, skip_gain, input_coeff, output_coeff, gate_input, mix_grad):
    doc_ext = jnp.concatenate([jnp.full((KERNEL - 1,), -1, jnp.int32), doc_ids])
    padded_all = jnp.concatenate([jnp.zeros((KERNEL - 1, INNER), jnp.float32), conv_input.astype(jnp.float32)])
    group_heads = SSM_HEADS // GROUPS
    blocks = SEQLEN // STRETCH
    zero_state = jnp.zeros((SSM_DIM, STATE), jnp.float32)
    start_doc = jnp.int32(-1)

    def forward(padded, weight, raw_step, bias_one, rate_one, skip_one, group_in, group_out, gate_part):
        head_act = conv_act(padded, doc_ext, weight)
        step_size = jax.nn.softplus(raw_step + bias_one)
        log_decay = -step_size * jnp.exp(rate_one)
        in_grid = group_in.reshape(blocks, STRETCH, STATE)
        out_grid = group_out.reshape(blocks, STRETCH, STATE)
        pair_grid = jnp.einsum('cin,cjn->cij', out_grid, in_grid, precision=EXACT)
        return head_output(head_act, step_size, log_decay, pair_grid, in_grid, out_grid, gate_part, skip_one, zero_state, doc_ids, start_doc)[0]

    def one_head(carry, head_index):
        sum_in, sum_out = carry
        column = head_index * SSM_DIM
        group_col = head_index // group_heads * STATE
        primals = (lax.dynamic_slice_in_dim(padded_all, column, SSM_DIM, 1), lax.dynamic_slice_in_dim(conv_weight, column, SSM_DIM, 1), lax.dynamic_index_in_dim(step_raw, head_index, 1, keepdims=False), step_bias[head_index], rate_log[head_index], skip_gain[head_index], lax.dynamic_slice_in_dim(input_coeff, group_col, STATE, 1).astype(jnp.float32), lax.dynamic_slice_in_dim(output_coeff, group_col, STATE, 1).astype(jnp.float32), lax.dynamic_slice_in_dim(gate_input, column, SSM_DIM, 1).astype(jnp.float32))
        cotangent = lax.dynamic_slice_in_dim(mix_grad, column, SSM_DIM, 1).astype(jnp.float32)
        gradients = jax.vjp(forward, *primals)[1](cotangent)
        sum_in = lax.dynamic_update_slice_in_dim(sum_in, lax.dynamic_slice_in_dim(sum_in, group_col, STATE, 1) + gradients[6], group_col, 1)
        sum_out = lax.dynamic_update_slice_in_dim(sum_out, lax.dynamic_slice_in_dim(sum_out, group_col, STATE, 1) + gradients[7], group_col, 1)
        return ((sum_in, sum_out), (gradients[0][KERNEL - 1:].astype(jnp.bfloat16), gradients[8].astype(jnp.bfloat16), gradients[2], gradients[1], gradients[3], gradients[4], gradients[5]))
    zero_cols = jnp.zeros((SEQLEN, GROUPS * STATE), jnp.float32)
    (sum_in, sum_out), stacked = lax.scan(one_head, (zero_cols, zero_cols), jnp.arange(SSM_HEADS, dtype=jnp.int32))
    conv_grad, gate_grad, step_grad, weight_grad, bias_grad, rate_grad, skip_grad = stacked
    grad_conv_input = jnp.transpose(conv_grad, (1, 0, 2)).reshape(SEQLEN, INNER)
    grad_gate = jnp.transpose(gate_grad, (1, 0, 2)).reshape(SEQLEN, INNER)
    grad_conv_weight = jnp.transpose(weight_grad, (1, 0, 2)).reshape(KERNEL, INNER)
    return (grad_conv_input, grad_gate, step_grad.T, sum_in, sum_out, grad_conv_weight, bias_grad, rate_grad, skip_grad)

def reference(queries, keys, values, attn_grad, doc_ids, conv_input, conv_weight, step_raw, step_bias, rate_log, skip_gain, input_coeff, output_coeff, gate_input, mix_grad):
    grad_queries, grad_keys, grad_values = attention_grads(queries, keys, values, attn_grad, doc_ids)
    grad_conv_input, grad_gate, grad_step, grad_input_coeff, grad_output_coeff, grad_conv_weight, grad_step_bias, grad_rate_log, grad_skip = mixer_grads(doc_ids, conv_input, conv_weight, step_raw, step_bias, rate_log, skip_gain, input_coeff, output_coeff, gate_input, mix_grad)
    return (grad_queries, grad_keys, grad_values, grad_conv_input, grad_gate, grad_step, grad_input_coeff, grad_output_coeff, grad_conv_weight, grad_step_bias, grad_rate_log, grad_skip)
```

```python
import functools

import jax
import jax.numpy as jnp
from jax import lax
from jax.experimental import pallas as pl
from jax.experimental.pallas import tpu as pltpu
from jax.sharding import PartitionSpec as P

HEAD_DIM = 224
WINDOW = 1024
SSM_HEADS = 112
STATE = 64
GROUPS = 2
KERNEL = 4
PAD = 8
LANES = 128

EXACT = lax.Precision.HIGHEST
F32 = jnp.float32
BF16 = jnp.bfloat16
NEG_FILL = -1e30


def passed_along(value, axis, steps):
    count = lax.axis_size(axis)
    initial, last = (max(0, -steps), min(count, count - steps))
    return lax.ppermute(value, axis, [(source, source + steps) for source in range(initial, last)])


def dot(a, b, ca, cb, precision=None):
    return lax.dot_general(
        a, b, (((ca,), (cb,)), ((), ())), preferred_element_type=F32, precision=precision
    )


def attention_kernel(reach, docq_ref, dock_ref, q_ref, do_ref, *refs):
    k_refs = refs[: reach + 1]
    v_refs = refs[reach + 1 : 2 * reach + 2]
    dq_ref = refs[2 * reach + 2]
    dk_refs = refs[2 * reach + 3 : 3 * reach + 4]
    dv_refs = refs[3 * reach + 4 : 4 * reach + 5]
    bias_ref = refs[4 * reach + 5]
    rows = q_ref.shape[1]

    @pl.when(pl.program_id(0) == 0)
    def _():
        for gap in range(reach + 1):
            j = lax.broadcasted_iota(jnp.int32, (rows, rows), 0)
            i = lax.broadcasted_iota(jnp.int32, (rows, rows), 1)
            distance = gap * rows + i - j
            same = dock_ref[gap * rows : (gap + 1) * rows, :] == docq_ref[...]
            allowed = (distance >= 0) & (distance < WINDOW) & same
            bias_ref[gap] = jnp.where(allowed, 0.0, NEG_FILL)

    q = q_ref[0]
    grad = do_ref[0]
    scale = HEAD_DIM ** (-0.5)
    scores = []
    top = None
    for gap in range(reach + 1):
        s = dot(k_refs[gap][0], q, 1, 1) * scale + bias_ref[gap]
        scores.append(s)
        m = jnp.max(s, axis=0, keepdims=True)
        top = m if top is None else jnp.maximum(top, m)
    total = None
    expo = []
    for gap in range(reach + 1):
        e = jnp.exp(scores[gap] - top)
        expo.append(e)
        t = jnp.sum(e, axis=0, keepdims=True)
        total = t if total is None else total + t
    inverse = 1.0 / jnp.maximum(total, 1.0)
    delta = None
    dprobs = []
    for gap in range(reach + 1):
        p = expo[gap] * inverse
        half = p.astype(BF16)
        dp = dot(v_refs[gap][0], grad, 1, 1)
        d = jnp.sum(half.astype(F32) * dp, axis=0, keepdims=True)
        delta = d if delta is None else delta + d
        dv = dot(half, grad, 1, 0)
        dv_refs[gap][0] = dv.astype(dv_refs[gap].dtype)
        dprobs.append(dp)
    dq = None
    for gap in range(reach + 1):
        ds = (expo[gap] * inverse * (dprobs[gap] - delta)).astype(BF16)
        dk = dot(ds, q, 1, 0)
        dk_refs[gap][0] = dk.astype(dk_refs[gap].dtype)
        part = dot(ds, k_refs[gap][0], 0, 0)
        dq = part if dq is None else dq + part
    dq_ref[0] = (dq * scale).astype(BF16)


def attention_call(docq, dock, q, grad, k_list, v_list):
    heads, rows, dim = q.shape
    reach = len(k_list) - 1
    head_spec = pl.BlockSpec((1, rows, dim), lambda h: (h, 0, 0))
    full = lambda shape: pl.BlockSpec(shape, lambda h: (0,) * len(shape))
    kinds = [F32] + [BF16] * reach
    shapes = [jax.ShapeDtypeStruct(q.shape, BF16)]
    shapes += [jax.ShapeDtypeStruct(q.shape, kind) for kind in kinds] * 2
    flops = 5 * 2 * heads * rows * rows * (reach + 1) * 256
    return pl.pallas_call(
        functools.partial(attention_kernel, reach),
        grid=(heads,),
        in_specs=[full(docq.shape), full(dock.shape)] + [head_spec] * (2 * reach + 4),
        out_specs=[head_spec] * (2 * reach + 3),
        out_shape=shapes,
        scratch_shapes=[pltpu.VMEM((reach + 1, rows, rows), F32)],
        name="attn",
        compiler_params=pltpu.CompilerParams(
            dimension_semantics=("arbitrary",), vmem_limit_bytes=56 * 1024 * 1024
        ),
        cost_estimate=pl.CostEstimate(
            flops=flops * 4, bytes_accessed=q.size * 2 * 24, transcendentals=0
        ),
    )(docq, dock, q, grad, *k_list, *v_list)


def pair_columns(cols, index, lower):
    return jnp.where(lower, cols[:, 2 * index : 2 * index + 1], cols[:, 2 * index + 1 : 2 * index + 2])


def conv_pre(conv_ref, tail_ref, wt_ref, mask_ref, xp_ref):
    rows = conv_ref.shape[0]
    xp_ref[:PAD, :] = tail_ref[...]
    xp_ref[PAD:, :] = conv_ref[...].astype(F32)
    pre = wt_ref[0:1, :] * xp_ref[PAD:, :]
    for lag in range(1, KERNEL):
        pre = pre + wt_ref[lag : lag + 1, :] * (xp_ref[PAD - lag : PAD - lag + rows, :] * mask_ref[lag - 1])
    return pre


def fill_masks(docm_ref, mask_ref):
    for lag in range(1, KERNEL):
        mask_ref[lag - 1] = jnp.broadcast_to(docm_ref[:, lag - 1 : lag], mask_ref.shape[1:])


def ends_kernel(
    docm_ref, b_ref, c_ref, conv_ref, tail_ref, wt_ref, gate_ref, mix_ref, cols_ref,
    end_ref, start_ref, mask_ref, xp_ref,
):
    @pl.when(pl.program_id(0) == 0)
    def _():
        fill_masks(docm_ref, mask_ref)

    rows = conv_ref.shape[0]
    lower = lax.broadcasted_iota(jnp.int32, (rows, LANES), 1) < LANES // 2
    cols = cols_ref[0]
    pre = conv_pre(conv_ref, tail_ref, wt_ref, mask_ref, xp_ref)
    act = pre * jax.nn.sigmoid(pre)
    weighted = act * pair_columns(cols, 1, lower) * pair_columns(cols, 3, lower)
    end_ref[...] = dot(b_ref[...], weighted.astype(BF16), 0, 0)
    gate = gate_ref[...].astype(F32)
    dy = mix_ref[...].astype(F32) * (gate * jax.nn.sigmoid(gate))
    start_ref[...] = dot(c_ref[...], (dy * pair_columns(cols, 2, lower)).astype(BF16), 0, 0)


def mixer_kernel(
    docm_ref, docc_ref, docr_ref, b_ref, c_ref, conv_ref, tail_ref, wt_ref, gate_ref, mix_ref,
    cols_ref, rowc_ref, state_ref, cot_ref,
    gconv_ref, edge_ref, ggate_ref, sums_ref, z_ref, u_ref, db_ref, dc_ref,
    mask_ref, xp_ref, bias_ref, pair_ref, dpair_ref, dpad_ref,
):
    step = pl.program_id(0)
    rows = conv_ref.shape[0]
    heads = z_ref.shape[1]

    @pl.when(step == 0)
    def _():
        fill_masks(docm_ref, mask_ref)
        i = lax.broadcasted_iota(jnp.int32, (rows, rows), 0)
        j = lax.broadcasted_iota(jnp.int32, (rows, rows), 1)
        bias_ref[...] = jnp.where((i >= j) & (docc_ref[...] == docr_ref[...]), 0.0, NEG_FILL)
        pair_ref[...] = dot(c_ref[...], b_ref[...], 1, 1)
        dpair_ref[...] = jnp.zeros_like(dpair_ref)
        db_ref[...] = jnp.zeros_like(db_ref)
        dc_ref[...] = jnp.zeros_like(dc_ref)
        z_ref[...] = jnp.zeros_like(z_ref)
        u_ref[...] = jnp.zeros_like(u_ref)
        dpad_ref[...] = jnp.zeros_like(dpad_ref)

    lower = lax.broadcasted_iota(jnp.int32, (rows, LANES), 1) < LANES // 2
    cols = cols_ref[0]
    size = pair_columns(cols, 1, lower)
    enter = pair_columns(cols, 2, lower)
    to_end = pair_columns(cols, 3, lower)
    pre = conv_pre(conv_ref, tail_ref, wt_ref, mask_ref, xp_ref)
    sig_pre = jax.nn.sigmoid(pre)
    act = pre * sig_pre
    x_half = (act * size).astype(BF16)
    gate = gate_ref[...].astype(F32)
    sig_gate = jax.nn.sigmoid(gate)
    silu_gate = gate * sig_gate
    cot = mix_ref[...].astype(F32)
    dy = cot * silu_gate
    dy_half = dy.astype(BF16)
    state = state_ref[...].astype(BF16)
    end_cot = cot_ref[...].astype(BF16)
    zero = jnp.zeros_like(dy_half)
    y_parts, dx_parts = [], []
    dpair = dpair_ref[...]
    for k in range(2):
        weights = jnp.exp((cols[:, k : k + 1] - rowc_ref[0, k : k + 1, :]) + bias_ref[...])
        mixing = (pair_ref[...] * weights).astype(BF16)
        y_parts.append(dot(mixing, x_half, 1, 0))
        dx_parts.append(dot(mixing, dy_half, 0, 0))
        dy_one = jnp.where(lower if k == 0 else ~lower, dy_half, zero)
        dpair = dpair + dot(dy_one, x_half, 1, 1) * weights
    dpair_ref[...] = dpair
    inner = jnp.where(lower, y_parts[0], y_parts[1]) + enter * dot(c_ref[...], state, 1, 0)
    end_part = to_end * dot(b_ref[...], end_cot, 1, 0)
    dx = jnp.where(lower, dx_parts[0], dx_parts[1]) + end_part
    skip = wt_ref[KERNEL : KERNEL + 1, :]
    y = inner + skip * act
    ggate_ref[...] = (cot * y * (sig_gate + silu_gate * (1.0 - sig_gate))).astype(BF16)
    x_wide = x_half.astype(F32)
    zed = dy_half.astype(F32) * inner - x_wide * dx
    you = dx * act
    lane = lax.broadcasted_iota(jnp.int32, (rows, heads), 1)
    for k in range(2):
        side = lower if k == 0 else ~lower
        here = lane == 2 * step + k
        z_one = jnp.sum(jnp.where(side, zed, 0.0), axis=1, keepdims=True)
        u_one = jnp.sum(jnp.where(side, you, 0.0), axis=1, keepdims=True)
        z_ref[...] = jnp.where(here, z_one, z_ref[...])
        u_ref[...] = jnp.where(here, u_one, u_ref[...])
    dc_ref[...] += dot((enter * dy).astype(BF16), state, 1, 1)
    db_ref[...] += dot((to_end * x_wide).astype(BF16), end_cot, 1, 1)
    dact = dx * size + skip * dy
    dpre = dact * (sig_pre + act * (1.0 - sig_pre))
    sums_ref[0:1, :] = jnp.sum(dpre * xp_ref[PAD:, :], axis=0, keepdims=True)
    dpad_ref[0, PAD : PAD + rows, :] = dpre
    grown = wt_ref[0:1, :] * dpad_ref[0, 0 : rows + PAD, :]
    for lag in range(1, KERNEL):
        masked = dpre * mask_ref[lag - 1]
        sums_ref[lag : lag + 1, :] = jnp.sum(
            masked * xp_ref[PAD - lag : PAD - lag + rows, :], axis=0, keepdims=True
        )
        dpad_ref[lag, PAD : PAD + rows, :] = masked
        grown = grown + wt_ref[lag : lag + 1, :] * dpad_ref[lag, lag : lag + rows + PAD, :]
    gconv_ref[...] = grown[PAD:, :].astype(BF16)
    edge_ref[0:PAD, :] = grown[:PAD, :]
    edge_ref[PAD:, :] = grown[rows:, :]
    sums_ref[4:5, :] = jnp.sum(dy * act, axis=0, keepdims=True)
    sums_ref[5:6, :] = jnp.sum(state.astype(F32) * end_cot.astype(F32), axis=0, keepdims=True)
    sums_ref[6:7, :] = jnp.sum(x_wide * end_part, axis=0, keepdims=True)
    sums_ref[7:8, :] = jnp.zeros((1, LANES), F32)

    @pl.when(step == pl.num_programs(0) - 1)
    def _():
        total = dpair_ref[...]
        dc_ref[...] += dot(total, b_ref[...].astype(F32), 1, 0, EXACT)
        db_ref[...] += dot(total, c_ref[...].astype(F32), 0, 0, EXACT)


def mixer_grads(
    doc_ids, conv_input, conv_weight, step_raw, step_bias, rate_log, skip_gain,
    input_coeff, output_coeff, gate_input, mix_grad,
):
    rows, heads = step_raw.shape
    channels = conv_input.shape[1]
    head_dim = channels // heads
    pairs = channels // LANES
    count, index = lax.axis_size("seq"), lax.axis_index("seq")
    doc_pad = jnp.concatenate([jnp.full((KERNEL - 1,), -1, jnp.int32), doc_ids])
    doc_ext = lax.dynamic_slice_in_dim(doc_pad, index * rows, rows + KERNEL - 1)
    doc_before = doc_ext[KERNEL - 2]
    doc_now = doc_ext[KERNEL - 1 :]
    docm = jnp.stack(
        [(doc_ext[KERNEL - 1 - k : KERNEL - 1 - k + rows] == doc_now) for k in range(1, KERNEL)], axis=1
    ).astype(F32)
    docc, docr = doc_now[:, None], doc_now[None, :]
    tail_rows = passed_along(conv_input[rows - KERNEL + 1 :], "seq", 1)
    tail = jnp.concatenate([jnp.zeros((PAD - KERNEL + 1, channels), F32), tail_rows.astype(F32)])
    group_index = lax.axis_index("head") * heads // (SSM_HEADS // GROUPS)
    group_in = lax.dynamic_slice_in_dim(input_coeff, group_index * STATE, STATE, 1)
    group_out = lax.dynamic_slice_in_dim(output_coeff, group_index * STATE, STATE, 1)
    raw = step_raw + step_bias
    step_size = jax.nn.softplus(raw)
    rate = jnp.exp(rate_log)
    log_decay = -step_size * rate
    t = jnp.arange(rows)
    tri = (t[:, None] >= t[None, :]).astype(F32)
    cum = jnp.dot(tri, log_decay, precision=EXACT)
    enter = jnp.where((doc_now == doc_before)[:, None], jnp.exp(cum), 0.0)
    to_end = jnp.where((doc_now == doc_now[-1])[:, None], jnp.exp(cum[-1:] - cum), 0.0)
    through = enter[-1]
    cols = jnp.stack([cum, step_size, enter, to_end])
    cols = cols.reshape(4, rows, pairs, 2).transpose(2, 1, 0, 3).reshape(pairs, rows, 8)
    rowc = cum.T.reshape(pairs, 2, rows)
    wt = jnp.concatenate(
        [conv_weight, jnp.repeat(skip_gain, head_dim)[None], jnp.zeros((7 - KERNEL, channels), F32)]
    )
    everything = lax.all_gather(through, "seq")

    wide = pl.BlockSpec((rows, LANES), lambda p: (0, p))
    eight = pl.BlockSpec((8, LANES), lambda p: (0, p))
    state_spec = pl.BlockSpec((STATE, LANES), lambda p: (0, p))
    cols_spec = pl.BlockSpec((1, rows, 8), lambda p: (p, 0, 0))
    rowc_spec = pl.BlockSpec((1, 2, rows), lambda p: (p, 0, 0))
    full = lambda a: pl.BlockSpec(a.shape, lambda p: (0,) * len(a.shape))
    struct = jax.ShapeDtypeStruct
    state_shape = struct((STATE, channels), F32)
    params = pltpu.CompilerParams(
        dimension_semantics=("arbitrary",), vmem_limit_bytes=48 * 1024 * 1024
    )
    local_end, start_grad = pl.pallas_call(
        ends_kernel,
        grid=(pairs,),
        in_specs=[full(docm), full(group_in), full(group_out), wide, eight, eight, wide, wide, cols_spec],
        out_specs=[state_spec, state_spec],
        out_shape=[state_shape, state_shape],
        scratch_shapes=[pltpu.VMEM((KERNEL - 1, rows, LANES), F32), pltpu.VMEM((rows + PAD, LANES), F32)],
        name="ends",
        compiler_params=params,
        cost_estimate=pl.CostEstimate(
            flops=pairs * 8_000_000_00 // 2, bytes_accessed=conv_input.size * 6, transcendentals=0
        ),
    )(docm, group_in, group_out, conv_input, tail, wt, gate_input, mix_grad, cols)

    span = max(1, count // 2)
    edge = jnp.zeros((span, heads), F32)
    padded = jnp.concatenate([edge, everything, edge])

    def product(first, number):
        window = lax.dynamic_slice_in_dim(padded, index + span + first, number)
        return jnp.repeat(jnp.prod(window, axis=0), head_dim)[None]

    state = passed_along(local_end.astype(BF16), "seq", 1)
    end_cot = passed_along(start_grad.astype(BF16), "seq", -1)
    reach = 1
    while reach < span:
        state_far = passed_along(state, "seq", reach)
        cot_far = passed_along(end_cot, "seq", -reach)
        state = (state.astype(F32) + product(-reach, reach) * state_far.astype(F32)).astype(BF16)
        end_cot = (end_cot.astype(F32) + product(1, reach) * cot_far.astype(F32)).astype(BF16)
        reach *= 2

    def finish():
        full_out = lambda shape: pl.BlockSpec(shape, lambda p: (0,) * len(shape))
        gconv, edges, ggate, sums, z, u, db, dc = pl.pallas_call(
            mixer_kernel,
            grid=(pairs,),
            in_specs=[
                full(docm), full(docc), full(docr), full(group_in), full(group_out),
                wide, eight, eight, wide, wide, cols_spec, rowc_spec, state_spec, state_spec,
            ],
            out_specs=[
                wide, pl.BlockSpec((2 * PAD, LANES), lambda p: (0, p)), wide, eight,
                full_out((rows, heads)), full_out((rows, heads)),
                full_out((rows, STATE)), full_out((rows, STATE)),
            ],
            out_shape=[
                struct((rows, channels), BF16), struct((2 * PAD, channels), F32),
                struct((rows, channels), BF16), struct((8, channels), F32),
                struct((rows, heads), F32), struct((rows, heads), F32),
                struct((rows, STATE), F32), struct((rows, STATE), F32),
            ],
            scratch_shapes=[
                pltpu.VMEM((KERNEL - 1, rows, LANES), F32),
                pltpu.VMEM((rows + PAD, LANES), F32),
                pltpu.VMEM((rows, rows), F32),
                pltpu.VMEM((rows, rows), F32),
                pltpu.VMEM((rows, rows), F32),
                pltpu.VMEM((KERNEL, rows + 2 * PAD, LANES), F32),
            ],
            name="mixer",
            compiler_params=params,
            cost_estimate=pl.CostEstimate(
                flops=pairs * 1_500_000_000, bytes_accessed=conv_input.size * 10, transcendentals=0
            ),
        )(
            docm, docc, docr, group_in, group_out, conv_input, tail, wt, gate_input, mix_grad,
            cols, rowc, state, end_cot,
        )
        spill = passed_along(edges[PAD - KERNEL + 1 : PAD], "seq", -1)
        last = (edges[2 * PAD - KERNEL + 1 :] + spill).astype(BF16)
        grad_conv_input = gconv.at[rows - KERNEL + 1 :].set(last)
        per_head = jnp.sum(sums[4:7].reshape(3, heads, head_dim), axis=2)
        last_row = per_head[2] + through * per_head[1]
        dcum = z + jnp.where((t == rows - 1)[:, None], last_row[None], 0.0)
        dlog = jnp.dot(tri.T, dcum, precision=EXACT)
        grad_step = (u - dlog * rate) * jax.nn.sigmoid(raw)
        zero_cols = jnp.zeros((2, rows, GROUPS * STATE), BF16)
        both = lax.dynamic_update_slice_in_dim(
            zero_cols, jnp.stack([db, dc]).astype(BF16), group_index * STATE, 2
        )
        both = lax.psum(both, "head").astype(F32)
        conv_total, bias_total, rate_total, skip_total = lax.psum(
            (sums[:KERNEL], jnp.sum(grad_step, axis=0), jnp.sum(dlog * log_decay, axis=0), per_head[0]),
            "seq",
        )
        return (
            grad_conv_input, ggate, grad_step, both[0], both[1],
            conv_total, bias_total, rate_total, skip_total,
        )

    return finish


def local(
    queries, keys, values, attn_grad, doc_ids, conv_input, conv_weight, step_raw, step_bias,
    rate_log, skip_gain, input_coeff, output_coeff, gate_input, mix_grad,
):
    rows, width = queries.shape
    heads = width // HEAD_DIM
    reach = WINDOW // rows
    split = lambda a: a.reshape(rows, heads, HEAD_DIM).transpose(1, 0, 2)
    k_own, v_own = split(keys), split(values)
    k_list, v_list = [k_own], [v_own]
    for gap in range(1, reach + 1):
        k_list.append(passed_along(k_own, "seq", gap))
        v_list.append(passed_along(v_own, "seq", gap))
    doc_wide = jnp.concatenate([jnp.full((WINDOW,), -1, jnp.int32), doc_ids])
    own_start = lax.axis_index("seq") * rows + WINDOW
    docs = [lax.dynamic_slice_in_dim(doc_wide, own_start - gap * rows, rows) for gap in range(reach + 1)]
    finish = mixer_grads(
        doc_ids, conv_input, conv_weight, step_raw, step_bias, rate_log, skip_gain,
        input_coeff, output_coeff, gate_input, mix_grad,
    )
    outs = attention_call(
        docs[0][None, :], jnp.concatenate(docs)[:, None], split(queries), split(attn_grad), k_list, v_list
    )
    dq, dk, dv = outs[0], outs[1 : reach + 2], outs[reach + 2 :]
    key_acc, value_acc = dk[0], dv[0]
    back = [
        (passed_along(dk[gap], "seq", -gap), passed_along(dv[gap], "seq", -gap))
        for gap in range(1, reach + 1)
    ]
    mixed = finish()
    for back_k, back_v in back:
        key_acc = key_acc + back_k.astype(F32)
        value_acc = value_acc + back_v.astype(F32)
    merge = lambda a: a.transpose(1, 0, 2).reshape(rows, width)
    grad_keys = merge((key_acc * HEAD_DIM ** (-0.5)).astype(BF16))
    return (merge(dq), grad_keys, merge(value_acc.astype(BF16)), *mixed)


def solution(mesh):
    sharded = P("seq", "head")
    return jax.shard_map(
        local,
        mesh=mesh,
        in_specs=(
            sharded, sharded, sharded, sharded, P(), sharded, P(None, "head"), sharded,
            P("head"), P("head"), P("head"), P("seq", None), P("seq", None), sharded, sharded,
        ),
        out_specs=(
            sharded, sharded, sharded, sharded, sharded, sharded,
            P("seq", None), P("seq", None), P(None, "head"), P("head"), P("head"), P("head"),
        ),
        check_vma=False,
    )
```

```python
import functools

import jax
import jax.numpy as jnp
from jax import lax
from jax.experimental import pallas as pl
from jax.experimental.pallas import tpu as pltpu
from jax.sharding import PartitionSpec as P

HEAD_DIM = 224
WINDOW = 1024
SSM_HEADS = 112
STATE = 64
GROUPS = 2
KERNEL = 4
PAD = 8
LANES = 128

EXACT = lax.Precision.HIGHEST
F32 = jnp.float32
BF16 = jnp.bfloat16
NEG_FILL = -1e30


def passed_along(value, axis, steps):
    count = lax.axis_size(axis)
    initial, last = (max(0, -steps), min(count, count - steps))
    return lax.ppermute(value, axis, [(source, source + steps) for source in range(initial, last)])


def dot(a, b, ca, cb, precision=None):
    return lax.dot_general(
        a, b, (((ca,), (cb,)), ((), ())), preferred_element_type=F32, precision=precision
    )


def attention_kernel(group, where_ref, docq_ref, dock_ref, *refs):
    main, back = refs[:group], refs[group : 2 * group]
    own_out, back_out = refs[2 * group : 3 * group], refs[3 * group : 4 * group]
    q_all, do_all, k_all, v_all, dq_all, dk_all, dv_all = refs[4 * group :]
    rows = main[0].shape[2]
    span = group * rows
    scale = HEAD_DIM ** (-0.5)
    for r in range(group):
        first = pl.multiple_of(where_ref[r] * rows, rows)
        here, later = pl.ds(first, rows), pl.ds(pl.multiple_of(first + span, rows), rows)
        q_all[here, :] = main[r][0, 0]
        do_all[here, :] = main[r][1, 0]
        k_all[later, :] = main[r][2, 0]
        v_all[later, :] = main[r][3, 0]
        k_all[here, :] = back[r][0, 0]
        v_all[here, :] = back[r][1, 0]
    dk_all[...] = jnp.zeros_like(dk_all)
    dv_all[...] = jnp.zeros_like(dv_all)
    j = lax.broadcasted_iota(jnp.int32, (rows, rows), 0)
    i = lax.broadcasted_iota(jnp.int32, (rows, rows), 1)

    def block(b, carry):
        mine = pl.ds(pl.multiple_of(b * rows, rows), rows)
        q = q_all[mine, :]
        grad = do_all[mine, :]
        docq = docq_ref[pl.ds(b, 1), :]
        places = [pl.ds(pl.multiple_of((b + group - gap) * rows, rows), rows) for gap in range(group + 1)]
        scores = []
        top = None
        for gap in range(group + 1):
            distance = gap * rows + i - j
            allowed = (distance >= 0) & (distance < WINDOW) & (dock_ref[places[gap], :] == docq)
            s = jnp.where(allowed, dot(k_all[places[gap], :], q, 1, 1) * scale, NEG_FILL)
            scores.append(s)
            m = jnp.max(s, axis=0, keepdims=True)
            top = m if top is None else jnp.maximum(top, m)
        total = None
        expo = []
        for gap in range(group + 1):
            e = jnp.exp(scores[gap] - top)
            expo.append(e)
            t = jnp.sum(e, axis=0, keepdims=True)
            total = t if total is None else total + t
        inverse = 1.0 / jnp.maximum(total, 1.0)
        delta = None
        dprobs = []
        for gap in range(group + 1):
            half = (expo[gap] * inverse).astype(BF16)
            dp = dot(v_all[places[gap], :], grad, 1, 1)
            d = jnp.sum(half.astype(F32) * dp, axis=0, keepdims=True)
            delta = d if delta is None else delta + d
            dv_all[places[gap], :] += dot(half, grad, 1, 0)
            dprobs.append(dp)
        dq = None
        for gap in range(group + 1):
            ds = (expo[gap] * inverse * (dprobs[gap] - delta)).astype(BF16)
            dk_all[places[gap], :] += dot(ds, q, 1, 0)
            part = dot(ds, k_all[places[gap], :], 0, 0)
            dq = part if dq is None else dq + part
        dq_all[mine, :] = (dq * scale).astype(BF16)
        return carry

    lax.fori_loop(0, group, block, 0)
    for r in range(group):
        first = pl.multiple_of(where_ref[r] * rows, rows)
        here, later = pl.ds(first, rows), pl.ds(pl.multiple_of(first + span, rows), rows)
        own_out[r][0, 0] = dq_all[here, :]
        own_out[r][1, 0] = dk_all[later, :].astype(BF16)
        own_out[r][2, 0] = dv_all[later, :].astype(BF16)
        back_out[r][0, 0] = dk_all[here, :].astype(BF16)
        back_out[r][1, 0] = dv_all[here, :].astype(BF16)


def attention_call(places, docq, dock, main, back):
    group = len(main)
    _, heads, rows, dim = main[0].shape
    part = lambda n: pl.BlockSpec((n, 1, rows, dim), lambda h: (0, h, 0, 0))
    full = lambda shape: pl.BlockSpec(shape, lambda h: (0,) * len(shape))
    struct = lambda n: jax.ShapeDtypeStruct((n, heads, rows, dim), BF16)
    flops = 5 * 2 * heads * group * rows * rows * (group + 1) * 256
    wide = (2 * group * rows, dim)
    half = (group * rows, dim)
    outs = pl.pallas_call(
        functools.partial(attention_kernel, group),
        grid=(heads,),
        in_specs=[pl.BlockSpec(memory_space=pltpu.SMEM), full(docq.shape), full(dock.shape)]
        + [part(4)] * group
        + [part(2)] * group,
        out_specs=[part(3)] * group + [part(2)] * group,
        out_shape=[struct(3)] * group + [struct(2)] * group,
        scratch_shapes=[
            pltpu.VMEM(half, BF16), pltpu.VMEM(half, BF16), pltpu.VMEM(wide, BF16), pltpu.VMEM(wide, BF16),
            pltpu.VMEM(half, BF16), pltpu.VMEM(wide, F32), pltpu.VMEM(wide, F32),
        ],
        name="attn",
        compiler_params=pltpu.CompilerParams(
            dimension_semantics=("arbitrary",), vmem_limit_bytes=56 * 1024 * 1024
        ),
        cost_estimate=pl.CostEstimate(
            flops=flops * 3, bytes_accessed=heads * group * rows * dim * 2 * 11, transcendentals=0
        ),
    )(places, docq, dock, *main, *back)
    return outs[:group], outs[group:]


def swapped(value, distance):
    count = lax.axis_size("seq")
    return lax.ppermute(value, "seq", [(s, s ^ distance) for s in range(count)])


def spread(stacked, group, place):
    part = stacked.shape[1] // group
    pieces = [
        lax.dynamic_slice_in_dim(stacked, (place ^ r) * part, part, 1) for r in range(group)
    ]
    return [pieces[0]] + [swapped(pieces[r], r) for r in range(1, group)]


def gathered(pieces, group, place):
    part = pieces[0].shape[1]
    number, _, rows, dim = pieces[0].shape
    whole = jnp.zeros((number, part * group, rows, dim), pieces[0].dtype)
    for r in range(group):
        piece = pieces[0] if r == 0 else swapped(pieces[r], r)
        whole = lax.dynamic_update_slice_in_dim(whole, piece, (place ^ r) * part, 1)
    return whole


def everywhere_sum(value):
    step = 1
    while step < lax.axis_size("seq"):
        value = value + swapped(value, step)
        step *= 2
    return value


def pair_columns(cols, index, lower):
    return jnp.where(lower, cols[:, 2 * index : 2 * index + 1], cols[:, 2 * index + 1 : 2 * index + 2])


def conv_pre(conv_ref, tail_ref, wt_ref, mask_ref, xp_ref):
    rows = conv_ref.shape[0]
    xp_ref[:PAD, :] = tail_ref[...]
    xp_ref[PAD:, :] = conv_ref[...].astype(F32)
    pre = wt_ref[0:1, :] * xp_ref[PAD:, :]
    for lag in range(1, KERNEL):
        pre = pre + wt_ref[lag : lag + 1, :] * (xp_ref[PAD - lag : PAD - lag + rows, :] * mask_ref[lag - 1])
    return pre


def fill_masks(docm_ref, mask_ref):
    for lag in range(1, KERNEL):
        mask_ref[lag - 1] = jnp.broadcast_to(docm_ref[:, lag - 1 : lag], mask_ref.shape[1:])


def ends_kernel(
    docm_ref, b_ref, c_ref, conv_ref, tail_ref, wt_ref, gate_ref, mix_ref, cols_ref,
    end_ref, start_ref, mask_ref, xp_ref,
):
    @pl.when(pl.program_id(0) == 0)
    def _():
        fill_masks(docm_ref, mask_ref)

    rows = conv_ref.shape[0]
    lower = lax.broadcasted_iota(jnp.int32, (rows, LANES), 1) < LANES // 2
    cols = cols_ref[0]
    pre = conv_pre(conv_ref, tail_ref, wt_ref, mask_ref, xp_ref)
    act = pre * jax.nn.sigmoid(pre)
    weighted = act * pair_columns(cols, 1, lower) * pair_columns(cols, 3, lower)
    end_ref[...] = dot(b_ref[...], weighted.astype(BF16), 0, 0)
    gate = gate_ref[...].astype(F32)
    dy = mix_ref[...].astype(F32) * (gate * jax.nn.sigmoid(gate))
    start_ref[...] = dot(c_ref[...], (dy * pair_columns(cols, 2, lower)).astype(BF16), 0, 0)


def mixer_kernel(
    docm_ref, docc_ref, docr_ref, b_ref, c_ref, conv_ref, tail_ref, wt_ref, gate_ref, mix_ref,
    cols_ref, rowc_ref, state_ref, cot_ref,
    gconv_ref, edge_ref, ggate_ref, sums_ref, z_ref, u_ref, db_ref, dc_ref,
    mask_ref, xp_ref, bias_ref, pair_ref, dpair_ref, dpad_ref,
):
    step = pl.program_id(0)
    rows = conv_ref.shape[0]
    heads = z_ref.shape[1]

    @pl.when(step == 0)
    def _():
        fill_masks(docm_ref, mask_ref)
        i = lax.broadcasted_iota(jnp.int32, (rows, rows), 0)
        j = lax.broadcasted_iota(jnp.int32, (rows, rows), 1)
        bias_ref[...] = jnp.where((i >= j) & (docc_ref[...] == docr_ref[...]), 0.0, NEG_FILL)
        pair_ref[...] = dot(c_ref[...], b_ref[...], 1, 1)
        dpair_ref[...] = jnp.zeros_like(dpair_ref)
        db_ref[...] = jnp.zeros_like(db_ref)
        dc_ref[...] = jnp.zeros_like(dc_ref)
        z_ref[...] = jnp.zeros_like(z_ref)
        u_ref[...] = jnp.zeros_like(u_ref)
        dpad_ref[...] = jnp.zeros_like(dpad_ref)

    lower = lax.broadcasted_iota(jnp.int32, (rows, LANES), 1) < LANES // 2
    cols = cols_ref[0]
    size = pair_columns(cols, 1, lower)
    enter = pair_columns(cols, 2, lower)
    to_end = pair_columns(cols, 3, lower)
    pre = conv_pre(conv_ref, tail_ref, wt_ref, mask_ref, xp_ref)
    sig_pre = jax.nn.sigmoid(pre)
    act = pre * sig_pre
    x_half = (act * size).astype(BF16)
    gate = gate_ref[...].astype(F32)
    sig_gate = jax.nn.sigmoid(gate)
    silu_gate = gate * sig_gate
    cot = mix_ref[...].astype(F32)
    dy = cot * silu_gate
    dy_half = dy.astype(BF16)
    state = state_ref[...].astype(BF16)
    end_cot = cot_ref[...].astype(BF16)
    zero = jnp.zeros_like(dy_half)
    y_parts, dx_parts = [], []
    dpair = dpair_ref[...]
    for k in range(2):
        weights = jnp.exp((cols[:, k : k + 1] - rowc_ref[0, k : k + 1, :]) + bias_ref[...])
        mixing = (pair_ref[...] * weights).astype(BF16)
        y_parts.append(dot(mixing, x_half, 1, 0))
        dx_parts.append(dot(mixing, dy_half, 0, 0))
        dy_one = jnp.where(lower if k == 0 else ~lower, dy_half, zero)
        dpair = dpair + dot(dy_one, x_half, 1, 1) * weights
    dpair_ref[...] = dpair
    inner = jnp.where(lower, y_parts[0], y_parts[1]) + enter * dot(c_ref[...], state, 1, 0)
    end_part = to_end * dot(b_ref[...], end_cot, 1, 0)
    dx = jnp.where(lower, dx_parts[0], dx_parts[1]) + end_part
    skip = wt_ref[KERNEL : KERNEL + 1, :]
    y = inner + skip * act
    ggate_ref[...] = (cot * y * (sig_gate + silu_gate * (1.0 - sig_gate))).astype(BF16)
    x_wide = x_half.astype(F32)
    zed = dy_half.astype(F32) * inner - x_wide * dx
    you = dx * act
    lane = lax.broadcasted_iota(jnp.int32, (rows, heads), 1)
    for k in range(2):
        side = lower if k == 0 else ~lower
        here = lane == 2 * step + k
        z_one = jnp.sum(jnp.where(side, zed, 0.0), axis=1, keepdims=True)
        u_one = jnp.sum(jnp.where(side, you, 0.0), axis=1, keepdims=True)
        z_ref[...] = jnp.where(here, z_one, z_ref[...])
        u_ref[...] = jnp.where(here, u_one, u_ref[...])
    dc_ref[...] += dot((enter * dy).astype(BF16), state, 1, 1)
    db_ref[...] += dot((to_end * x_wide).astype(BF16), end_cot, 1, 1)
    dact = dx * size + skip * dy
    dpre = dact * (sig_pre + act * (1.0 - sig_pre))
    sums_ref[0:1, :] = jnp.sum(dpre * xp_ref[PAD:, :], axis=0, keepdims=True)
    dpad_ref[0, PAD : PAD + rows, :] = dpre
    grown = wt_ref[0:1, :] * dpad_ref[0, 0 : rows + PAD, :]
    for lag in range(1, KERNEL):
        masked = dpre * mask_ref[lag - 1]
        sums_ref[lag : lag + 1, :] = jnp.sum(
            masked * xp_ref[PAD - lag : PAD - lag + rows, :], axis=0, keepdims=True
        )
        dpad_ref[lag, PAD : PAD + rows, :] = masked
        grown = grown + wt_ref[lag : lag + 1, :] * dpad_ref[lag, lag : lag + rows + PAD, :]
    gconv_ref[...] = grown[PAD:, :].astype(BF16)
    edge_ref[0:PAD, :] = grown[:PAD, :]
    edge_ref[PAD:, :] = grown[rows:, :]
    sums_ref[4:5, :] = jnp.sum(dy * act, axis=0, keepdims=True)
    sums_ref[5:6, :] = jnp.sum(state.astype(F32) * end_cot.astype(F32), axis=0, keepdims=True)
    sums_ref[6:7, :] = jnp.sum(x_wide * end_part, axis=0, keepdims=True)
    sums_ref[7:8, :] = jnp.zeros((1, LANES), F32)

    @pl.when(step == pl.num_programs(0) - 1)
    def _():
        total = dpair_ref[...]
        dc_ref[...] += dot(total, b_ref[...].astype(F32), 1, 0, EXACT)
        db_ref[...] += dot(total, c_ref[...].astype(F32), 0, 0, EXACT)


def mixer_grads(
    doc_ids, conv_input, conv_weight, step_raw, step_bias, rate_log, skip_gain,
    input_coeff, output_coeff, gate_input, mix_grad,
):
    rows, heads = step_raw.shape
    channels = conv_input.shape[1]
    head_dim = channels // heads
    pairs = channels // LANES
    count, index = lax.axis_size("seq"), lax.axis_index("seq")
    doc_pad = jnp.concatenate([jnp.full((KERNEL - 1,), -1, jnp.int32), doc_ids])
    doc_ext = lax.dynamic_slice_in_dim(doc_pad, index * rows, rows + KERNEL - 1)
    doc_before = doc_ext[KERNEL - 2]
    doc_now = doc_ext[KERNEL - 1 :]
    docm = jnp.stack(
        [(doc_ext[KERNEL - 1 - k : KERNEL - 1 - k + rows] == doc_now) for k in range(1, KERNEL)], axis=1
    ).astype(F32)
    docc, docr = doc_now[:, None], doc_now[None, :]
    tail_rows = passed_along(conv_input[rows - KERNEL + 1 :], "seq", 1)
    tail = jnp.concatenate([jnp.zeros((PAD - KERNEL + 1, channels), F32), tail_rows.astype(F32)])
    group_index = lax.axis_index("head") * heads // (SSM_HEADS // GROUPS)
    group_in = lax.dynamic_slice_in_dim(input_coeff, group_index * STATE, STATE, 1)
    group_out = lax.dynamic_slice_in_dim(output_coeff, group_index * STATE, STATE, 1)
    raw = step_raw + step_bias
    step_size = jax.nn.softplus(raw)
    rate = jnp.exp(rate_log)
    log_decay = -step_size * rate
    t = jnp.arange(rows)
    tri = (t[:, None] >= t[None, :]).astype(F32)
    cum = jnp.dot(tri, log_decay, precision=EXACT)
    enter = jnp.where((doc_now == doc_before)[:, None], jnp.exp(cum), 0.0)
    to_end = jnp.where((doc_now == doc_now[-1])[:, None], jnp.exp(cum[-1:] - cum), 0.0)
    through = enter[-1]
    cols = jnp.stack([cum, step_size, enter, to_end])
    cols = cols.reshape(4, rows, pairs, 2).transpose(2, 1, 0, 3).reshape(pairs, rows, 8)
    rowc = cum.T.reshape(pairs, 2, rows)
    wt = jnp.concatenate(
        [conv_weight, jnp.repeat(skip_gain, head_dim)[None], jnp.zeros((7 - KERNEL, channels), F32)]
    )

    wide = pl.BlockSpec((rows, LANES), lambda p: (0, p))
    eight = pl.BlockSpec((8, LANES), lambda p: (0, p))
    state_spec = pl.BlockSpec((STATE, LANES), lambda p: (0, p))
    cols_spec = pl.BlockSpec((1, rows, 8), lambda p: (p, 0, 0))
    rowc_spec = pl.BlockSpec((1, 2, rows), lambda p: (p, 0, 0))
    full = lambda a: pl.BlockSpec(a.shape, lambda p: (0,) * len(a.shape))
    struct = jax.ShapeDtypeStruct
    state_shape = struct((STATE, channels), F32)
    params = pltpu.CompilerParams(
        dimension_semantics=("arbitrary",), vmem_limit_bytes=48 * 1024 * 1024
    )
    local_end, start_grad = pl.pallas_call(
        ends_kernel,
        grid=(pairs,),
        in_specs=[full(docm), full(group_in), full(group_out), wide, eight, eight, wide, wide, cols_spec],
        out_specs=[state_spec, state_spec],
        out_shape=[state_shape, state_shape],
        scratch_shapes=[pltpu.VMEM((KERNEL - 1, rows, LANES), F32), pltpu.VMEM((rows + PAD, LANES), F32)],
        name="ends",
        compiler_params=params,
        cost_estimate=pl.CostEstimate(
            flops=pairs * 8_000_000_00 // 2, bytes_accessed=conv_input.size * 6, transcendentals=0
        ),
    )(docm, group_in, group_out, conv_input, tail, wt, gate_input, mix_grad, cols)

    span = max(1, count // 2)
    grow = lambda factor: jnp.repeat(factor, head_dim)[None]
    state = passed_along(local_end.astype(BF16), "seq", 1)
    end_cot = passed_along(start_grad.astype(BF16), "seq", -1)
    decay, decay_back = passed_along(through, "seq", 1), passed_along(through, "seq", -1)
    reach = 1
    while reach < span:
        state_far = passed_along(state, "seq", reach)
        cot_far = passed_along(end_cot, "seq", -reach)
        state = (state.astype(F32) + grow(decay) * state_far.astype(F32)).astype(BF16)
        end_cot = (end_cot.astype(F32) + grow(decay_back) * cot_far.astype(F32)).astype(BF16)
        if 2 * reach < span:
            decay = decay * passed_along(decay, "seq", reach)
            decay_back = decay_back * passed_along(decay_back, "seq", -reach)
        reach *= 2

    def finish():
        full_out = lambda shape: pl.BlockSpec(shape, lambda p: (0,) * len(shape))
        gconv, edges, ggate, sums, z, u, db, dc = pl.pallas_call(
            mixer_kernel,
            grid=(pairs,),
            in_specs=[
                full(docm), full(docc), full(docr), full(group_in), full(group_out),
                wide, eight, eight, wide, wide, cols_spec, rowc_spec, state_spec, state_spec,
            ],
            out_specs=[
                wide, pl.BlockSpec((2 * PAD, LANES), lambda p: (0, p)), wide, eight,
                full_out((rows, heads)), full_out((rows, heads)),
                full_out((rows, STATE)), full_out((rows, STATE)),
            ],
            out_shape=[
                struct((rows, channels), BF16), struct((2 * PAD, channels), F32),
                struct((rows, channels), BF16), struct((8, channels), F32),
                struct((rows, heads), F32), struct((rows, heads), F32),
                struct((rows, STATE), F32), struct((rows, STATE), F32),
            ],
            scratch_shapes=[
                pltpu.VMEM((KERNEL - 1, rows, LANES), F32),
                pltpu.VMEM((rows + PAD, LANES), F32),
                pltpu.VMEM((rows, rows), F32),
                pltpu.VMEM((rows, rows), F32),
                pltpu.VMEM((rows, rows), F32),
                pltpu.VMEM((KERNEL, rows + 2 * PAD, LANES), F32),
            ],
            name="mixer",
            compiler_params=params,
            cost_estimate=pl.CostEstimate(
                flops=pairs * 1_500_000_000, bytes_accessed=conv_input.size * 10, transcendentals=0
            ),
        )(
            docm, docc, docr, group_in, group_out, conv_input, tail, wt, gate_input, mix_grad,
            cols, rowc, state, end_cot,
        )
        spill = passed_along(edges[PAD - KERNEL + 1 : PAD], "seq", -1)
        last = (edges[2 * PAD - KERNEL + 1 :] + spill).astype(BF16)
        grad_conv_input = gconv.at[rows - KERNEL + 1 :].set(last)
        per_head = jnp.sum(sums[4:7].reshape(3, heads, head_dim), axis=2)
        last_row = per_head[2] + through * per_head[1]
        dcum = z + jnp.where((t == rows - 1)[:, None], last_row[None], 0.0)
        dlog = jnp.dot(tri.T, dcum, precision=EXACT)
        grad_step = (u - dlog * rate) * jax.nn.sigmoid(raw)
        zero_cols = jnp.zeros((2, rows, GROUPS * STATE), BF16)
        both = lax.dynamic_update_slice_in_dim(
            zero_cols, jnp.stack([db, dc]).astype(BF16), group_index * STATE, 2
        )
        both = lax.psum(both, "head").astype(F32)
        small = jnp.concatenate(
            [jnp.sum(grad_step, axis=0), jnp.sum(dlog * log_decay, axis=0), per_head[0]]
        )
        small = jnp.pad(small, (0, channels - 3 * heads))
        total = everywhere_sum(jnp.concatenate([sums[:KERNEL], small[None]]))
        conv_total = total[:KERNEL]
        bias_total, rate_total, skip_total = total[KERNEL, : 3 * heads].reshape(3, heads)
        return (
            grad_conv_input, ggate, grad_step, both[0], both[1],
            conv_total, bias_total, rate_total, skip_total,
        )

    return finish


def local(
    queries, keys, values, attn_grad, doc_ids, conv_input, conv_weight, step_raw, step_bias,
    rate_log, skip_gain, input_coeff, output_coeff, gate_input, mix_grad,
):
    rows, width = queries.shape
    heads = width // HEAD_DIM
    group = WINDOW // rows
    index = lax.axis_index("seq")
    place = index % group
    split = lambda a: a.reshape(rows, heads, HEAD_DIM).transpose(1, 0, 2)
    stacked = jnp.stack([split(queries), split(attn_grad), split(keys), split(values)])
    before = passed_along(stacked[2:], "seq", group)
    main = spread(stacked, group, place)
    back = spread(before, group, place)
    doc_wide = jnp.concatenate([jnp.full((WINDOW,), -1, jnp.int32), doc_ids])
    dock = lax.dynamic_slice_in_dim(doc_wide, (index - place) * rows, 2 * WINDOW)
    docq = dock[WINDOW:].reshape(group, rows)
    finish = mixer_grads(
        doc_ids, conv_input, conv_weight, step_raw, step_bias, rate_log, skip_gain,
        input_coeff, output_coeff, gate_input, mix_grad,
    )
    places = place ^ jnp.arange(group, dtype=jnp.int32)
    own_out, back_out = attention_call(places, docq, dock[:, None], main, back)
    returned = passed_along(gathered(back_out, group, place), "seq", -group)
    own = gathered(own_out, group, place)
    mixed = finish()
    merge = lambda a: a.transpose(1, 0, 2).reshape(rows, width)
    grad_keys = (own[1].astype(F32) + returned[0].astype(F32)) * HEAD_DIM ** (-0.5)
    grad_values = own[2].astype(F32) + returned[1].astype(F32)
    return (merge(own[0]), merge(grad_keys.astype(BF16)), merge(grad_values.astype(BF16)), *mixed)


def solution(mesh):
    sharded = P("seq", "head")
    return jax.shard_map(
        local,
        mesh=mesh,
        in_specs=(
            sharded, sharded, sharded, sharded, P(), sharded, P(None, "head"), sharded,
            P("head"), P("head"), P("head"), P("seq", None), P("seq", None), sharded, sharded,
        ),
        out_specs=(
            sharded, sharded, sharded, sharded, sharded, sharded,
            P("seq", None), P("seq", None), P(None, "head"), P("head"), P("head"), P("head"),
        ),
        check_vma=False,
    )
```
